32 devices in a mesh: dp: 8 (over z, y), tensor: 4 (over x, core).
Axes of the slice: x: 2, y: 2, z: 4, core: 2. Of those that a mesh axis runs over, the one named last changes fastest.
Arguments:
- hidden_a: bfloat16 [768, 8192], P(('dp', 'tensor')), parts along dimension 0, may hold values from -120 to 120
- hidden_b: bfloat16 [768, 8192], P(('dp', 'tensor')), parts along dimension 0, may hold values from -120 to 120
- grad_out: float32 [768], P(('dp', 'tensor')), parts along dimension 0, may hold values from -40 to 40
- head_weight: bfloat16 [8192, 2560], P(None, 'tensor'), may hold values from -0.1875 to 0.1875
Outputs:
- entropy_b: float32 [768], P(('dp', 'tensor')), parts along dimension 0
- grad_a: bfloat16 [768, 8192], P(('dp', 'tensor')), parts along dimension 0
The draws below stay inside these ranges and needn't reach their ends.
There are 8 independent parts, one for each index of `dp`. The reference program is written for one: setup_inputs(seed, part) draws one part's arguments, and reference() takes and returns one part's arrays. A program takes and returns all parts, laid end to end along the dimension named above; an argument that names none is the same for every part. Nothing has to cross between parts.
All inputs are finite; a program needn't handle non-finite values.
Results may differ from the reference program's by a relative error of at most 0.018.
Values may be sent and summed in bfloat16 or wider, within the bound.
No kernel may reach another device: no remote copies, remote signals or barrier semaphores. Data moves between devices by JAX's collectives and lax.ppermute only.
A program may use at most 64 MiB of HBM per device.

```python
import jax
import jax.numpy as jnp
from jax import lax

D = 8192
VSH = 640
TOKENS = 96
VOCAB = 2560
N_TENSOR = 4


def hidden_rows(key):
    base = jnp.clip(jax.random.normal(jax.random.fold_in(key, 1), (TOKENS, D), jnp.float32), -6.0, 6.0)
    return base.astype(jnp.bfloat16)


def draw_hidden_a(key, part):
    return hidden_rows(jax.random.fold_in(key, 101))


def draw_hidden_b(key, part):
    return hidden_rows(jax.random.fold_in(key, 202))


def levels(key, shape, pieces, smallest, high):
    def one(axis_at, shards_of):
        heights = jax.random.uniform(jax.random.fold_in(jax.random.fold_in(key, 6), axis_at), (shards_of,), jnp.float32, smallest / len(pieces), high / len(pieces))
        return jnp.repeat(jnp.exp(heights), shape[axis_at] // shards_of).reshape((-1,) + (1,) * (len(shape) - axis_at - 1))

    gain = one(*pieces[0])
    for cut in pieces[1:]:
        gain = gain * one(*cut)
    return gain


def gaussian(rng, extent, deviation, bound, cuts=(), dtype=jnp.bfloat16):
    drawn = deviation * jax.random.normal(rng, extent, jnp.float32)
    if cuts:
        drawn = drawn * levels(rng, extent, cuts, -0.22, 0.18)
    return jnp.clip(drawn, -bound, bound).astype(dtype)


def setup_inputs(seed: int = 0, part: int = 0) -> dict:
    seeds = jax.random.split(jax.random.key(seed), 5)
    part_splits = jax.random.split(jax.random.fold_in(seeds[4], part), 5)
    return {
        "hidden_a": draw_hidden_a(jax.random.fold_in(jax.random.fold_in(seeds[4], part), 71), part),
        "hidden_b": draw_hidden_b(jax.random.fold_in(jax.random.fold_in(seeds[4], part), 71), part),
        "grad_out": gaussian(part_splits[2], (TOKENS,), 8.0, 40.0, ((0, 4),), jnp.float32),
        "head_weight": gaussian(seeds[3], (D, VOCAB), (D // 9) ** -0.5, 0.1875, ((1, 4),)),
    }


def span_stats(logits):
    peak = jnp.max(logits, axis=1, keepdims=True)
    shifted = logits - peak
    powers = jnp.exp(shifted)
    total = jnp.sum(powers, axis=1)
    moment = jnp.sum(powers * shifted, axis=1)
    return shifted, powers, total, moment


def reference(hidden_a, hidden_b, grad_out, head_weight):
    logits_a = jnp.dot(hidden_a, head_weight, preferred_element_type=jnp.float32)
    logits_b = jnp.dot(hidden_b, head_weight, preferred_element_type=jnp.float32)
    stats_b = span_stats(logits_b)
    entropy_b = jnp.log(stats_b[2]) - stats_b[3] / stats_b[2]
    shifted_a, powers_a, total_a, moment_a = span_stats(logits_a)
    scaled = -(powers_a / total_a[:, None]) * (shifted_a - (moment_a / total_a)[:, None])
    scaled = scaled.astype(jnp.bfloat16)

    def add_shard(index, carry):
        start = (index * VSH).astype(jnp.int32)
        columns = lax.dynamic_slice_in_dim(scaled, start, VSH, 1)
        weights = lax.dynamic_slice_in_dim(head_weight, start, VSH, 1)
        partial_sum = lax.dot_general(columns, weights, (((1,), (1,)), ((), ())), preferred_element_type=jnp.float32)
        rounded = lax.optimization_barrier(partial_sum.astype(jnp.bfloat16))
        return carry + rounded.astype(jnp.float32)

    summed = lax.fori_loop(jnp.int32(0), jnp.int32(N_TENSOR), add_shard, jnp.zeros((TOKENS, D), jnp.float32))
    grad_a = (grad_out[:, None] * summed).astype(jnp.bfloat16)
    return (entropy_b, grad_a)
```

```python
import functools

import jax
import jax.numpy as jnp
from jax import lax
from jax.experimental import pallas as pl
from jax.experimental.pallas import tpu as pltpu
from jax.sharding import PartitionSpec as P


CHUNK = 1024
PAD = 32
A_SHARES = (8,)
B_SHARES = (5, 3)
G_SHARES = (3, 5)
T_PARTS = 4
VMEM_LIMIT = 24 * 1024 * 1024
STAGE_LIMIT = 40 * 1024 * 1024


def vmem_spec():
    return pl.BlockSpec(memory_space=pltpu.VMEM)


def columns_to_rows(columns):
    count = columns[0].shape[0]
    lane = lax.broadcasted_iota(jnp.int32, (count, 128), 1)
    packed = jnp.zeros((count, 128), jnp.float32)
    for index, column in enumerate(columns):
        packed = jnp.where(lane == index, column, packed)
    return jnp.transpose(packed)[:8]


def rows_to_columns(rows):
    count = rows[0].shape[1]
    sub = lax.broadcasted_iota(jnp.int32, (128, count), 0)
    packed = jnp.zeros((128, count), jnp.float32)
    for index, row in enumerate(rows):
        packed = jnp.where(sub == index, row, packed)
    turned = jnp.transpose(packed)
    return [turned[:, index : index + 1] for index in range(len(rows))]


def spans(shares, depth):
    edges = [0]
    for share in shares:
        edges.append(edges[-1] + depth * share // sum(shares))
    return list(zip(edges, edges[1:]))


def logits_kernel(ranges, slots, more, last, *refs):
    held = len(ranges) * slots
    pieces, weight, sums, outs = refs[:held], refs[held], refs[held + 1 : held + 1 + more], refs[held + 1 + more :]
    logits = sums[0][...] if more else None
    for part, (low, high) in enumerate(ranges):
        for start in range(low, high, CHUNK):
            stop = min(start + CHUNK, high)
            rows = []
            for ref in pieces[part * slots : (part + 1) * slots]:
                offset = start if ref.shape[1] > high - low else start - low
                rows.append(ref[:, offset : offset + stop - start])
                rows.append(jnp.zeros((PAD - ref.shape[0], stop - start), jnp.bfloat16))
            left = jnp.concatenate(rows, axis=0)
            product = jnp.dot(left, weight[start:stop, :], preferred_element_type=jnp.float32)
            logits = product if logits is None else logits + product
    if not last:
        outs[0][...] = logits
        return
    peak = jnp.max(logits, axis=1, keepdims=True)
    shifted = logits - peak
    powers = jnp.exp(shifted)
    total = jnp.sum(powers, axis=1, keepdims=True)
    moment = jnp.sum(powers * shifted, axis=1, keepdims=True)
    outs[0][...] = columns_to_rows([peak, total, moment])
    if len(outs) > 1:
        outs[1][...] = logits


def logits_and_stats(ranges, pieces, weight, sums, last, with_logits):
    slots, vocab = len(pieces) // len(ranges), weight.shape[1]
    out = [jax.ShapeDtypeStruct((slots * PAD, vocab), jnp.float32)]
    if last:
        out = [jax.ShapeDtypeStruct((8, slots * PAD), jnp.float32)] + (out if with_logits else [])
    return call(functools.partial(logits_kernel, ranges, slots, len(sums), last), out, *pieces, weight, *sums)


def align_lanes(stats, shift, flip, chips):
    half = chips * PAD
    if flip:
        stats = pltpu.roll(stats, half, 1)
    move = shift * PAD
    if move:
        lane = lax.broadcasted_iota(jnp.int32, stats.shape, 1) % half
        stats = jnp.where(lane < move, pltpu.roll(stats, (move - half) % (2 * half), 1), pltpu.roll(stats, move, 1))
    return stats


def combine(everyone):
    peak = everyone[0][0:1]
    for stats in everyone[1:]:
        peak = jnp.maximum(peak, stats[0:1])
    total = jnp.zeros_like(peak)
    moment = jnp.zeros_like(peak)
    for stats in everyone:
        below = stats[0:1] - peak
        scale = jnp.exp(below)
        total = total + scale * stats[1:2]
        moment = moment + scale * (stats[2:3] + below * stats[1:2])
    return peak, total, moment


def combine_chips(chips, refs):
    shifted = [align_lanes(ref[...], shift, 0, chips) for shift, ref in enumerate(refs)]
    return combine(shifted)


def pair_stats_kernel(chips, own, mate, out):
    values = combine([own[...], align_lanes(mate[...], 0, 1, chips)])
    out[...] = jnp.concatenate([*values, jnp.zeros((5, out.shape[1]), jnp.float32)], axis=0)


def partial_product(scaled, turned, low, rows, chips, keep, send):
    half, width = turned[0].shape[1], keep.shape[1]
    start = low
    while start < low + width:
        stop = min(low + width, (start // half + 1) * half)
        right = turned[start // half][:, start % half : start % half + stop - start]
        product = jnp.dot(scaled, right, preferred_element_type=jnp.float32)
        for slot in range(chips):
            place = slice(slot * rows, (slot + 1) * rows), slice(start - low, stop - low)
            keep[place] = product[slot * PAD : slot * PAD + rows]
            high = (chips + slot) * PAD
            send[place] = product[high : high + rows].astype(jnp.bfloat16)
        start = stop


def first_gradient_kernel(rows, chips, low, logits, *refs):
    stats, turned = refs[:chips], refs[chips : chips + T_PARTS]
    scaled_out, keep, send = refs[chips + T_PARTS :]
    peak, total, moment = combine_chips(chips, stats)
    peak, inverse, mean = rows_to_columns([peak, 1.0 / total, moment / total])
    shifted = logits[...] - peak
    scaled = -(jnp.exp(shifted) * inverse) * (shifted - mean)
    scaled = scaled.astype(jnp.bfloat16)
    scaled_out[...] = scaled
    partial_product(scaled, turned, low, rows, chips, keep, send)


def gradient_kernel(rows, chips, low, scaled, *refs):
    partial_product(scaled[...], refs[:T_PARTS], low, rows, chips, *refs[T_PARTS:])


def gradient_shapes(rows, chips, width):
    return [
        jax.ShapeDtypeStruct((chips * rows, width), jnp.float32),
        jax.ShapeDtypeStruct((chips * rows, width), jnp.bfloat16),
    ]


def pair_sum_kernel(rows, chips, keep, received, *outs):
    outs[0][...] = keep[0:rows, :] + received[0:rows, :].astype(jnp.float32)
    for slot in range(1, chips):
        low = slot * rows
        total = keep[low : low + rows, :] + received[low : low + rows, :].astype(jnp.float32)
        outs[slot][...] = total.astype(jnp.bfloat16)


def finish_kernel(parts, chips, factor, *refs):
    others = chips - 1
    out, entropy = refs[-2:]
    scale = factor[...]
    low = 0
    for part in range(parts):
        total = refs[part][...]
        for other in range(others):
            total = total + refs[parts + part * others + other][...].astype(jnp.float32)
        out[:, low : low + total.shape[1]] = (scale * total).astype(jnp.bfloat16)
        low += total.shape[1]
    _, total, moment = combine_chips(chips, refs[parts * chips : parts * chips + chips])
    entropy[...] = (jnp.log(total) - moment / total)[0, : entropy.shape[0]]


def call(kernel, out, *args):
    return pl.pallas_call(
        kernel,
        out_shape=out,
        in_specs=[vmem_spec()] * len(args),
        out_specs=jax.tree.map(lambda _: vmem_spec(), out),
        compiler_params=pltpu.CompilerParams(vmem_limit_bytes=VMEM_LIMIT),
    )(*args)


def stage_kernel(weight, out, semaphores):
    steps = semaphores.shape[0]
    step = out.shape[0] // steps
    copies = []
    for index in range(steps):
        part = pl.ds(index * step, step)
        copies.append(pltpu.make_async_copy(weight.at[part, :], out.at[part, :], semaphores.at[index]))
        copies[-1].start()
    for copy in copies:
        copy.wait()


def stage(weight):
    return pl.pallas_call(
        stage_kernel,
        out_shape=jax.ShapeDtypeStruct(weight.shape, weight.dtype),
        in_specs=[pl.BlockSpec(memory_space=pl.ANY)],
        out_specs=vmem_spec(),
        scratch_shapes=[pltpu.SemaphoreType.DMA((4,))],
        compiler_params=pltpu.CompilerParams(vmem_limit_bytes=STAGE_LIMIT),
        name="stage",
    )(weight)


def turn_kernel(low, weight, turned):
    vocab, size = turned.shape
    for column in range(0, vocab, 256):
        block = min(256, vocab - column)
        one = lax.broadcasted_iota(jnp.int32, (block, block), 0) == lax.broadcasted_iota(jnp.int32, (block, block), 1)
        flipped = lax.dot_general(
            jnp.where(one, 1.0, 0.0).astype(jnp.bfloat16),
            weight[low : low + size, column : column + block],
            (((1,), (1,)), ((), ())),
            preferred_element_type=jnp.float32,
        )
        turned[column : column + block, :] = flipped.astype(jnp.bfloat16)


def per_device(chips, hidden_a, hidden_b, grad_out, head_weight):
    rows, depth = hidden_a.shape

    def move(array, shift, flip):
        pairs = [
            (2 * chip + core, 2 * ((chip + shift) % chips) + (core ^ flip)) for chip in range(chips) for core in range(2)
        ]
        return lax.ppermute(array, "tensor", pairs)

    def pair_stats(stats):
        mate = move(stats, 0, 1)
        chip = call(
            functools.partial(pair_stats_kernel, chips), jax.ShapeDtypeStruct(stats.shape, jnp.float32), stats, mate
        )
        return [chip] + [move(chip, shift, 0) for shift in range(1, chips)]

    def gather(hidden, shares):
        ranges, parts = spans(shares, depth), []
        own = [hidden if high - low == depth else hidden[:, low:high] for low, high in ranges]
        mate = move(hidden, 0, 1)
        for piece in own:
            across = [move(piece, shift, 0) for shift in range(1, chips)]
            relayed = [move(p, 0, 1) for p in across]
            parts.append([hidden, *across, mate, *relayed])
        return ranges, parts

    ranges_a, parts_a = gather(hidden_a, A_SHARES)
    ranges_b, parts_b = gather(hidden_b, B_SHARES)
    vocab = head_weight.shape[1]
    weight = stage(head_weight)
    turned, size = [], depth // T_PARTS
    for index in range(T_PARTS):
        turned.append(
            call(
                functools.partial(turn_kernel, index * size), jax.ShapeDtypeStruct((vocab, size), weight.dtype), weight
            )
        )

    def all_logits(ranges, parts, with_logits):
        sums = []
        for index, (span, part) in enumerate(zip(ranges, parts)):
            sums = logits_and_stats([span], part, weight, sums, index == len(parts) - 1, with_logits)
        return sums

    stats_a, logits_a = all_logits(ranges_a, parts_a, True)
    chips_a = pair_stats(stats_a)

    kept, arrived = [], []
    for index, (low, high) in enumerate(spans(G_SHARES, depth)):
        width = high - low
        if index == 0:
            scaled, keep, send = call(
                functools.partial(first_gradient_kernel, rows, chips, low),
                [jax.ShapeDtypeStruct((2 * chips * PAD, vocab), jnp.bfloat16)] + gradient_shapes(rows, chips, width),
                logits_a,
                *chips_a,
                *turned,
            )
        else:
            keep, send = call(
                functools.partial(gradient_kernel, rows, chips, low),
                gradient_shapes(rows, chips, width),
                scaled,
                *turned,
            )
        received = move(send, 0, 1)
        sums = call(
            functools.partial(pair_sum_kernel, rows, chips),
            [jax.ShapeDtypeStruct((rows, width), jnp.float32)]
            + [jax.ShapeDtypeStruct((rows, width), jnp.bfloat16)] * (chips - 1),
            keep,
            received,
        )
        kept.append(sums[0])
        arrived.append([move(p, chips - shift, 0) for shift, p in zip(range(1, chips), sums[1:])])

    (stats_b,) = all_logits(ranges_b, parts_b, False)
    chips_b = pair_stats(stats_b)
    grad_a, entropy = call(
        functools.partial(finish_kernel, len(G_SHARES), chips),
        [jax.ShapeDtypeStruct((rows, depth), jnp.bfloat16), jax.ShapeDtypeStruct((rows,), jnp.float32)],
        grad_out[:, None],
        *kept,
        *[p for ps in arrived for p in ps],
        *chips_b,
    )
    return entropy, grad_a


def solution(mesh):
    chips = mesh.shape["tensor"] // 2
    placed = (
        P(("dp", "tensor"), None),
        P(("dp", "tensor"), None),
        P(("dp", "tensor")),
        P(None, "tensor"),
    )

    def body(*args):
        return per_device(chips, *args)

    return jax.shard_map(
        body,
        mesh=mesh,
        in_specs=placed,
        out_specs=(P(("dp", "tensor")), P(("dp", "tensor"), None)),
        check_vma=False,
    )
```

```python
import functools

import jax
import jax.numpy as jnp
from jax import lax
from jax.experimental import pallas as pl
from jax.experimental.pallas import tpu as pltpu
from jax.sharding import PartitionSpec as P


CHUNK = 1024
PAD = 32
A_SHARES = (8,)
B_SHARES = (13, 3)
G_SHARES = (4, 4)
T_PARTS = 4
VMEM_LIMIT = 24 * 1024 * 1024
STAGE_LIMIT = 40 * 1024 * 1024


def vmem_spec():
    return pl.BlockSpec(memory_space=pltpu.VMEM)


def columns_to_rows(columns):
    count = columns[0].shape[0]
    lane = lax.broadcasted_iota(jnp.int32, (count, 128), 1)
    packed = jnp.zeros((count, 128), jnp.float32)
    for index, column in enumerate(columns):
        packed = jnp.where(lane == index, column, packed)
    return jnp.transpose(packed)[:8]


def rows_to_columns(rows):
    count = rows[0].shape[1]
    sub = lax.broadcasted_iota(jnp.int32, (128, count), 0)
    packed = jnp.zeros((128, count), jnp.float32)
    for index, row in enumerate(rows):
        packed = jnp.where(sub == index, row, packed)
    turned = jnp.transpose(packed)
    return [turned[:, index : index + 1] for index in range(len(rows))]


def spans(shares, depth):
    edges = [0]
    for share in shares:
        edges.append(edges[-1] + depth * share // sum(shares))
    return list(zip(edges, edges[1:]))


def logits_kernel(ranges, slots, more, last, *refs):
    held = len(ranges) * slots
    pieces, weight, sums, outs = refs[:held], refs[held], refs[held + 1 : held + 1 + more], refs[held + 1 + more :]
    logits = sums[0][...] if more else None
    for part, (low, high) in enumerate(ranges):
        for start in range(low, high, CHUNK):
            stop = min(start + CHUNK, high)
            rows = []
            for ref in pieces[part * slots : (part + 1) * slots]:
                offset = start if ref.shape[1] > high - low else start - low
                rows.append(ref[:, offset : offset + stop - start])
                rows.append(jnp.zeros((PAD - ref.shape[0], stop - start), jnp.bfloat16))
            left = jnp.concatenate(rows, axis=0)
            product = jnp.dot(left, weight[start:stop, :], preferred_element_type=jnp.float32)
            logits = product if logits is None else logits + product
    if not last:
        outs[0][...] = logits
        return
    peak = jnp.max(logits, axis=1, keepdims=True)
    shifted = logits - peak
    powers = jnp.exp(shifted)
    total = jnp.sum(powers, axis=1, keepdims=True)
    moment = jnp.sum(powers * shifted, axis=1, keepdims=True)
    outs[0][...] = columns_to_rows([peak, total, moment])
    if len(outs) > 1:
        count = logits.shape[0]
        outs[1][...] = logits
        outs[2][:count, :] = (powers * (shifted - moment / total)).astype(jnp.bfloat16)
        outs[2][count:, :] = powers.astype(jnp.bfloat16)


def logits_and_stats(ranges, pieces, weight, sums, last, with_logits):
    slots, vocab = len(pieces) // len(ranges), weight.shape[1]
    out = [jax.ShapeDtypeStruct((slots * PAD, vocab), jnp.float32)]
    if last:
        factors = jax.ShapeDtypeStruct((2 * slots * PAD, vocab), jnp.bfloat16)
        out = [jax.ShapeDtypeStruct((8, slots * PAD), jnp.float32)] + ([*out, factors] if with_logits else [])
    return call(functools.partial(logits_kernel, ranges, slots, len(sums), last), out, *pieces, weight, *sums)


def align_lanes(stats, shift, flip, chips):
    half = chips * PAD
    if flip:
        stats = pltpu.roll(stats, half, 1)
    move = shift * PAD
    if move:
        lane = lax.broadcasted_iota(jnp.int32, stats.shape, 1) % half
        stats = jnp.where(lane < move, pltpu.roll(stats, (move - half) % (2 * half), 1), pltpu.roll(stats, move, 1))
    return stats


def combine(everyone):
    peak = everyone[0][0:1]
    for stats in everyone[1:]:
        peak = jnp.maximum(peak, stats[0:1])
    total = jnp.zeros_like(peak)
    moment = jnp.zeros_like(peak)
    for stats in everyone:
        below = stats[0:1] - peak
        scale = jnp.exp(below)
        total = total + scale * stats[1:2]
        moment = moment + scale * (stats[2:3] + below * stats[1:2])
    return peak, total, moment


def combine_chips(chips, refs):
    shifted = [align_lanes(ref[...], shift, 0, chips) for shift, ref in enumerate(refs)]
    return combine(shifted)


def combine_cores(chips, refs):
    return combine([align_lanes(ref[...], index // 2, index % 2, chips) for index, ref in enumerate(refs)])


def pair_stats_kernel(chips, own, mate, out):
    values = combine([own[...], align_lanes(mate[...], 0, 1, chips)])
    out[...] = jnp.concatenate([*values, jnp.zeros((5, out.shape[1]), jnp.float32)], axis=0)


def partial_product(scaled, turned, low, rows, chips, keep, send):
    half, width = turned[0].shape[1], keep.shape[1]
    start = low
    while start < low + width:
        stop = min(low + width, (start // half + 1) * half)
        right = turned[start // half][:, start % half : start % half + stop - start]
        product = jnp.dot(scaled, right, preferred_element_type=jnp.float32)
        for slot in range(chips):
            place = slice(slot * rows, (slot + 1) * rows), slice(start - low, stop - low)
            keep[place] = product[slot * PAD : slot * PAD + rows]
            high = (chips + slot) * PAD
            send[place] = product[high : high + rows].astype(jnp.bfloat16)
        start = stop


def early_kernel(rows, chips, low, factors, *refs):
    turned, keep, send = refs[:T_PARTS], refs[-2], refs[-1]
    half, width = turned[0].shape[1], keep.shape[1]
    count = factors.shape[0] // 2
    for start in range(low, low + width, half):
        stop = min(low + width, start + half)
        product = jnp.dot(factors[...], turned[start // half][:, : stop - start], preferred_element_type=jnp.float32)
        for which in range(2):
            for slot in range(chips):
                place = (which * chips + slot) * rows
                near = which * count + slot * PAD
                far = near + chips * PAD
                keep[place : place + rows, start - low : stop - low] = product[near : near + rows]
                send[place : place + rows, start - low : stop - low] = product[far : far + rows].astype(jnp.bfloat16)


def late_kernel(rows, chips, keep, received, *refs):
    peak, total, moment = combine_cores(chips, refs[: 2 * chips])
    outs = refs[2 * chips :]
    factors = []
    for stats in (refs[0][...], align_lanes(refs[1][...], 0, 1, chips)):
        below = stats[0:1] - peak
        scale = -jnp.exp(below) / total
        factors += [scale, scale * (stats[2:3] / stats[1:2] + below - moment / total)]
    columns = rows_to_columns(factors)
    for slot in range(chips):
        total = None
        for which in range(4):
            source = (keep, received)[which // 2]
            place = (which % 2 * chips + slot) * rows
            column = columns[which][slot * PAD : slot * PAD + rows]
            term = column * source[place : place + rows, :].astype(jnp.float32)
            total = term if total is None else total + term
        outs[slot][...] = total.astype(outs[slot].dtype)


def gradient_kernel(rows, chips, low, logits, *refs):
    stats, refs = refs[: 2 * chips], refs[2 * chips :]
    turned, outs = refs[:T_PARTS], refs[T_PARTS:]
    peak, total, moment = combine_cores(chips, stats)
    peak, inverse, mean = rows_to_columns([peak, 1.0 / total, moment / total])
    shifted = logits[...] - peak
    scaled = -(jnp.exp(shifted) * inverse) * (shifted - mean)
    partial_product(scaled.astype(jnp.bfloat16), turned, low, rows, chips, *outs)


def gradient_shapes(rows, chips, width):
    return [
        jax.ShapeDtypeStruct((chips * rows, width), jnp.float32),
        jax.ShapeDtypeStruct((chips * rows, width), jnp.bfloat16),
    ]


def pair_sum_kernel(rows, chips, keep, received, *outs):
    outs[0][...] = keep[0:rows, :] + received[0:rows, :].astype(jnp.float32)
    for slot in range(1, chips):
        low = slot * rows
        total = keep[low : low + rows, :] + received[low : low + rows, :].astype(jnp.float32)
        outs[slot][...] = total.astype(jnp.bfloat16)


def finish_kernel(parts, chips, factor, *refs):
    others = chips - 1
    out, entropy = refs[-2:]
    scale = factor[...]
    low = 0
    for part in range(parts):
        total = refs[part][...]
        for other in range(others):
            total = total + refs[parts + part * others + other][...].astype(jnp.float32)
        out[:, low : low + total.shape[1]] = (scale * total).astype(jnp.bfloat16)
        low += total.shape[1]
    _, total, moment = combine_chips(chips, refs[parts * chips : parts * chips + chips])
    entropy[...] = (jnp.log(total) - moment / total)[0, : entropy.shape[0]]


def call(kernel, out, *args):
    return pl.pallas_call(
        kernel,
        out_shape=out,
        in_specs=[vmem_spec()] * len(args),
        out_specs=jax.tree.map(lambda _: vmem_spec(), out),
        compiler_params=pltpu.CompilerParams(vmem_limit_bytes=VMEM_LIMIT),
    )(*args)


def stage_kernel(weight, out, semaphores):
    steps = semaphores.shape[0]
    step = out.shape[0] // steps
    copies = []
    for index in range(steps):
        part = pl.ds(index * step, step)
        copies.append(pltpu.make_async_copy(weight.at[part, :], out.at[part, :], semaphores.at[index]))
        copies[-1].start()
    for copy in copies:
        copy.wait()


def stage(weight):
    return pl.pallas_call(
        stage_kernel,
        out_shape=jax.ShapeDtypeStruct(weight.shape, weight.dtype),
        in_specs=[pl.BlockSpec(memory_space=pl.ANY)],
        out_specs=vmem_spec(),
        scratch_shapes=[pltpu.SemaphoreType.DMA((4,))],
        compiler_params=pltpu.CompilerParams(vmem_limit_bytes=STAGE_LIMIT),
        name="stage",
    )(weight)


def turn_kernel(low, weight, turned):
    vocab, size = turned.shape
    for column in range(0, vocab, 256):
        block = min(256, vocab - column)
        one = lax.broadcasted_iota(jnp.int32, (block, block), 0) == lax.broadcasted_iota(jnp.int32, (block, block), 1)
        flipped = lax.dot_general(
            jnp.where(one, 1.0, 0.0).astype(jnp.bfloat16),
            weight[low : low + size, column : column + block],
            (((1,), (1,)), ((), ())),
            preferred_element_type=jnp.float32,
        )
        turned[column : column + block, :] = flipped.astype(jnp.bfloat16)


def per_device(chips, hidden_a, hidden_b, grad_out, head_weight):
    rows, depth = hidden_a.shape

    def move(array, shift, flip):
        pairs = [
            (2 * chip + core, 2 * ((chip + shift) % chips) + (core ^ flip)) for chip in range(chips) for core in range(2)
        ]
        return lax.ppermute(array, "tensor", pairs)

    def pair_stats(stats):
        mate = move(stats, 0, 1)
        chip = call(
            functools.partial(pair_stats_kernel, chips), jax.ShapeDtypeStruct(stats.shape, jnp.float32), stats, mate
        )
        return [chip] + [move(chip, shift, 0) for shift in range(1, chips)]

    def gather(hidden, shares):
        ranges, parts = spans(shares, depth), []
        own = [hidden if high - low == depth else hidden[:, low:high] for low, high in ranges]
        mate = move(hidden, 0, 1)
        for piece in own:
            across = [move(piece, shift, 0) for shift in range(1, chips)]
            relayed = [move(p, 0, 1) for p in across]
            parts.append([hidden, *across, mate, *relayed])
        return ranges, parts

    ranges_a, parts_a = gather(hidden_a, A_SHARES)
    ranges_b, parts_b = gather(hidden_b, B_SHARES)
    vocab = head_weight.shape[1]
    weight = stage(head_weight)
    turned, size = [], depth // T_PARTS
    for index in range(T_PARTS):
        turned.append(
            call(
                functools.partial(turn_kernel, index * size), jax.ShapeDtypeStruct((vocab, size), weight.dtype), weight
            )
        )

    def all_logits(ranges, parts, with_logits):
        sums = []
        for index, (span, part) in enumerate(zip(ranges, parts)):
            sums = logits_and_stats([span], part, weight, sums, index == len(parts) - 1, with_logits)
        return sums

    stats_a, logits_a, factors_a = all_logits(ranges_a, parts_a, True)
    across = [move(stats_a, shift, 0) for shift in range(1, chips)]
    cores_a = [stats_a, move(stats_a, 0, 1)]
    for piece in across:
        cores_a += [piece, move(piece, 0, 1)]

    kept, arrived = [], []
    for index, (low, high) in enumerate(spans(G_SHARES, depth)):
        width = high - low
        sums_shape = [jax.ShapeDtypeStruct((rows, width), jnp.float32)] + [
            jax.ShapeDtypeStruct((rows, width), jnp.bfloat16)
        ] * (chips - 1)
        held_shape = gradient_shapes((2 if index == 0 else 1) * rows, chips, width)
        if index == 0:
            keep, send = call(functools.partial(early_kernel, rows, chips, low), held_shape, factors_a, *turned)
        else:
            keep, send = call(
                functools.partial(gradient_kernel, rows, chips, low), held_shape, logits_a, *cores_a, *turned
            )
        received = move(send, 0, 1)
        if index == 0:
            sums = call(functools.partial(late_kernel, rows, chips), sums_shape, keep, received, *cores_a)
        else:
            sums = call(functools.partial(pair_sum_kernel, rows, chips), sums_shape, keep, received)
        kept.append(sums[0])
        arrived.append([move(p, chips - shift, 0) for shift, p in zip(range(1, chips), sums[1:])])

    (stats_b,) = all_logits(ranges_b, parts_b, False)
    chips_b = pair_stats(stats_b)
    grad_a, entropy = call(
        functools.partial(finish_kernel, len(G_SHARES), chips),
        [jax.ShapeDtypeStruct((rows, depth), jnp.bfloat16), jax.ShapeDtypeStruct((rows,), jnp.float32)],
        grad_out[:, None],
        *kept,
        *[p for ps in arrived for p in ps],
        *chips_b,
    )
    return entropy, grad_a


def solution(mesh):
    chips = mesh.shape["tensor"] // 2
    placed = (
        P(("dp", "tensor"), None),
        P(("dp", "tensor"), None),
        P(("dp", "tensor")),
        P(None, "tensor"),
    )

    def body(*args):
        return per_device(chips, *args)

    return jax.shard_map(
        body,
        mesh=mesh,
        in_specs=placed,
        out_specs=(P(("dp", "tensor")), P(("dp", "tensor"), None)),
        check_vma=False,
    )
```

```python
import functools

import jax
import jax.numpy as jnp
from jax import lax
from jax.experimental import pallas as pl
from jax.experimental.pallas import tpu as pltpu
from jax.sharding import PartitionSpec as P


CHUNK = 1024
PAD = 32
A_SHARES = (8,)
B_SHARES = (8,)
G_SHARES = (4, 4)
T_PARTS = 4
VMEM_LIMIT = 24 * 1024 * 1024
STAGE_LIMIT = 40 * 1024 * 1024


def vmem_spec():
    return pl.BlockSpec(memory_space=pltpu.VMEM)


def columns_to_rows(columns):
    count = columns[0].shape[0]
    lane = lax.broadcasted_iota(jnp.int32, (count, 128), 1)
    packed = jnp.zeros((count, 128), jnp.float32)
    for index, column in enumerate(columns):
        packed = jnp.where(lane == index, column, packed)
    return jnp.transpose(packed)[:8]


def rows_to_columns(rows):
    count = rows[0].shape[1]
    sub = lax.broadcasted_iota(jnp.int32, (128, count), 0)
    packed = jnp.zeros((128, count), jnp.float32)
    for index, row in enumerate(rows):
        packed = jnp.where(sub == index, row, packed)
    turned = jnp.transpose(packed)
    return [turned[:, index : index + 1] for index in range(len(rows))]


def spans(shares, depth):
    edges = [0]
    for share in shares:
        edges.append(edges[-1] + depth * share // sum(shares))
    return list(zip(edges, edges[1:]))


def logits_kernel(ranges, slots, more, last, *refs):
    held = len(ranges) * slots
    pieces, weight, sums, outs = refs[:held], refs[held], refs[held + 1 : held + 1 + more], refs[held + 1 + more :]
    logits = sums[0][...] if more else None
    for part, (low, high) in enumerate(ranges):
        for start in range(low, high, CHUNK):
            stop = min(start + CHUNK, high)
            rows = []
            for ref in pieces[part * slots : (part + 1) * slots]:
                offset = start if ref.shape[1] > high - low else start - low
                rows.append(ref[:, offset : offset + stop - start])
                rows.append(jnp.zeros((PAD - ref.shape[0], stop - start), jnp.bfloat16))
            left = jnp.concatenate(rows, axis=0)
            product = jnp.dot(left, weight[start:stop, :], preferred_element_type=jnp.float32)
            logits = product if logits is None else logits + product
    if not last:
        outs[0][...] = logits
        return
    peak = jnp.max(logits, axis=1, keepdims=True)
    shifted = logits - peak
    powers = jnp.exp(shifted)
    total = jnp.sum(powers, axis=1, keepdims=True)
    moment = jnp.sum(powers * shifted, axis=1, keepdims=True)
    outs[0][...] = columns_to_rows([peak, total, moment])
    if len(outs) > 1:
        outs[1][...] = logits
        around = (powers * (shifted - moment / total)).astype(jnp.bfloat16)
        powers = powers.astype(jnp.bfloat16)
        chips = slots // 2
        place = 0
        for first in (1, chips + 1):
            for values in (around, powers):
                size = (chips - 1) * PAD
                outs[2][place : place + size, :] = values[first * PAD : first * PAD + size]
                place += size


def logits_and_stats(ranges, pieces, weight, sums, last, with_logits):
    slots, vocab = len(pieces) // len(ranges), weight.shape[1]
    out = [jax.ShapeDtypeStruct((slots * PAD, vocab), jnp.float32)]
    if last:
        factors = jax.ShapeDtypeStruct((2 * (slots - 2) * PAD, vocab), jnp.bfloat16)
        out = [jax.ShapeDtypeStruct((8, slots * PAD), jnp.float32)] + ([*out, factors] if with_logits else [])
    return call(functools.partial(logits_kernel, ranges, slots, len(sums), last), out, *pieces, weight, *sums)


def align_lanes(stats, shift, flip, chips):
    half = chips * PAD
    if flip:
        stats = pltpu.roll(stats, half, 1)
    move = shift * PAD
    if move:
        lane = lax.broadcasted_iota(jnp.int32, stats.shape, 1) % half
        stats = jnp.where(lane < move, pltpu.roll(stats, (move - half) % (2 * half), 1), pltpu.roll(stats, move, 1))
    return stats


def combine(everyone):
    peak = everyone[0][0:1]
    for stats in everyone[1:]:
        peak = jnp.maximum(peak, stats[0:1])
    total = jnp.zeros_like(peak)
    moment = jnp.zeros_like(peak)
    for stats in everyone:
        below = stats[0:1] - peak
        scale = jnp.exp(below)
        total = total + scale * stats[1:2]
        moment = moment + scale * (stats[2:3] + below * stats[1:2])
    return peak, total, moment


def combine_chips(chips, refs):
    shifted = [align_lanes(ref[...], shift, 0, chips) for shift, ref in enumerate(refs)]
    return combine(shifted)


def combine_cores(chips, refs):
    return combine([align_lanes(ref[...], index // 2, index % 2, chips) for index, ref in enumerate(refs)])


def pair_stats_kernel(chips, own, mate, out):
    values = combine([own[...], align_lanes(mate[...], 0, 1, chips)])
    out[...] = jnp.concatenate([*values, jnp.zeros((5, out.shape[1]), jnp.float32)], axis=0)


def columns_of(turned, low, width):
    half, start = turned[0].shape[1], low
    while start < low + width:
        stop = min(low + width, (start // half + 1) * half)
        yield start - low, stop - low, turned[start // half][:, start % half : start % half + stop - start]
        start = stop


def early_kernel(rows, low, factors, *refs):
    turned, keep, send = refs[:T_PARTS], refs[-2], refs[-1]
    count = factors.shape[0] // 2
    for start, stop, right in columns_of(turned, low, keep.shape[1]):
        product = jnp.dot(factors[...], right, preferred_element_type=jnp.float32)
        for index in range(count // PAD):
            place = slice(index * rows, (index + 1) * rows)
            near, far = index * PAD, count + index * PAD
            keep[place, start:stop] = product[near : near + rows]
            send[place, start:stop] = product[far : far + rows].astype(jnp.bfloat16)


def late_kernel(rows, chips, keep, received, *refs):
    peak, total, moment = combine_cores(chips, refs[: 2 * chips])
    outs = refs[2 * chips :]
    factors = []
    for stats in (refs[0][...], align_lanes(refs[1][...], 0, 1, chips)):
        below = stats[0:1] - peak
        scale = -jnp.exp(below) / total
        factors += [scale, scale * (stats[2:3] / stats[1:2] + below - moment / total)]
    columns = rows_to_columns(factors)
    for slot in range(1, chips):
        total = None
        for which in range(4):
            source = (keep, received)[which // 2]
            place = (which % 2 * (chips - 1) + slot - 1) * rows
            column = columns[which][slot * PAD : slot * PAD + rows]
            term = column * source[place : place + rows, :].astype(jnp.float32)
            total = term if total is None else total + term
        outs[slot - 1][...] = total.astype(jnp.bfloat16)


def own_kernel(rows, chips, logits, *refs):
    stats, turned, outs = refs[: 2 * chips], refs[2 * chips : -3], refs[-3:]
    values = rows_to_columns(list(combine_cores(chips, stats)))
    scaled = []
    for first in (0, chips * PAD):
        peak, total, moment = (value[first : first + PAD] for value in values)
        shifted = logits[first : first + PAD, :] - peak
        scaled.append(-(jnp.exp(shifted) / total) * (shifted - moment / total))
    outs[0][...] = jnp.concatenate(scaled, axis=0).astype(jnp.bfloat16)
    more_own_kernel(rows, 0, outs[0], *turned, *outs[1:])


def more_own_kernel(rows, low, scaled, *refs):
    turned, keep, send = refs[:T_PARTS], refs[-2], refs[-1]
    for start, stop, right in columns_of(turned, low, keep.shape[1]):
        product = jnp.dot(scaled[...], right, preferred_element_type=jnp.float32)
        keep[:, start:stop] = product[:rows]
        send[:, start:stop] = product[PAD : PAD + rows].astype(jnp.bfloat16)


def finish_kernel(chips, factor, *refs):
    stats, parts, out, entropy = refs[:chips], refs[chips:-2], refs[-2], refs[-1]
    scale = factor[...]
    low = 0
    for first in range(0, len(parts), chips + 1):
        columns = slice(low, low + parts[first].shape[1])
        total = parts[first][...]
        for part in parts[first + 1 : first + chips + 1]:
            total = total + part[...].astype(jnp.float32)
        out[:, columns] = (scale * total).astype(jnp.bfloat16)
        low = columns.stop
    _, total, moment = combine_chips(chips, stats)
    entropy[...] = (jnp.log(total) - moment / total)[0, : entropy.shape[0]]


def held_shapes(rows, width):
    return [jax.ShapeDtypeStruct((rows, width), jnp.float32), jax.ShapeDtypeStruct((rows, width), jnp.bfloat16)]


def call(kernel, out, *args):
    return pl.pallas_call(
        kernel,
        out_shape=out,
        in_specs=[vmem_spec()] * len(args),
        out_specs=jax.tree.map(lambda _: vmem_spec(), out),
        compiler_params=pltpu.CompilerParams(vmem_limit_bytes=VMEM_LIMIT),
    )(*args)


def stage_kernel(weight, out, semaphores):
    steps = semaphores.shape[0]
    step = out.shape[0] // steps
    copies = []
    for index in range(steps):
        part = pl.ds(index * step, step)
        copies.append(pltpu.make_async_copy(weight.at[part, :], out.at[part, :], semaphores.at[index]))
        copies[-1].start()
    for copy in copies:
        copy.wait()


def stage(weight):
    return pl.pallas_call(
        stage_kernel,
        out_shape=jax.ShapeDtypeStruct(weight.shape, weight.dtype),
        in_specs=[pl.BlockSpec(memory_space=pl.ANY)],
        out_specs=vmem_spec(),
        scratch_shapes=[pltpu.SemaphoreType.DMA((4,))],
        compiler_params=pltpu.CompilerParams(vmem_limit_bytes=STAGE_LIMIT),
        name="stage",
    )(weight)


def turn_kernel(low, weight, turned):
    vocab, size = turned.shape
    for column in range(0, vocab, 256):
        block = min(256, vocab - column)
        one = lax.broadcasted_iota(jnp.int32, (block, block), 0) == lax.broadcasted_iota(jnp.int32, (block, block), 1)
        flipped = lax.dot_general(
            jnp.where(one, 1.0, 0.0).astype(jnp.bfloat16),
            weight[low : low + size, column : column + block],
            (((1,), (1,)), ((), ())),
            preferred_element_type=jnp.float32,
        )
        turned[column : column + block, :] = flipped.astype(jnp.bfloat16)


def per_device(chips, hidden_a, hidden_b, grad_out, head_weight):
    rows, depth = hidden_a.shape

    def move(array, shift, flip):
        pairs = [
            (2 * chip + core, 2 * ((chip + shift) % chips) + (core ^ flip)) for chip in range(chips) for core in range(2)
        ]
        return lax.ppermute(array, "tensor", pairs)

    def pair_stats(stats):
        mate = move(stats, 0, 1)
        chip = call(
            functools.partial(pair_stats_kernel, chips), jax.ShapeDtypeStruct(stats.shape, jnp.float32), stats, mate
        )
        return [chip] + [move(chip, shift, 0) for shift in range(1, chips)]

    def gather(hidden, shares):
        ranges, parts = spans(shares, depth), []
        own = [hidden if high - low == depth else hidden[:, low:high] for low, high in ranges]
        mate = move(hidden, 0, 1)
        for piece in own:
            across = [move(piece, shift, 0) for shift in range(1, chips)]
            relayed = [move(p, 0, 1) for p in across]
            parts.append([hidden, *across, mate, *relayed])
        return ranges, parts

    ranges_a, parts_a = gather(hidden_a, A_SHARES)
    ranges_b, parts_b = gather(hidden_b, B_SHARES)
    vocab = head_weight.shape[1]
    weight = stage(head_weight)
    turned, size = [], depth // T_PARTS
    for index in range(T_PARTS):
        turned.append(
            call(
                functools.partial(turn_kernel, index * size), jax.ShapeDtypeStruct((vocab, size), weight.dtype), weight
            )
        )

    def all_logits(ranges, parts, with_logits):
        sums = []
        for index, (span, part) in enumerate(zip(ranges, parts)):
            sums = logits_and_stats([span], part, weight, sums, index == len(parts) - 1, with_logits)
        return sums

    stats_a, logits_a, factors_a = all_logits(ranges_a, parts_a, True)
    across = [move(stats_a, shift, 0) for shift in range(1, chips)]
    cores_a = [stats_a, move(stats_a, 0, 1)]
    for shift, piece in enumerate(across, 1):
        cores_a += [piece, move(stats_a, shift, 1)]

    arrived = []
    for low, high in spans(G_SHARES, depth):
        width = high - low
        keep, send = call(
            functools.partial(early_kernel, rows, low), held_shapes(2 * (chips - 1) * rows, width), factors_a, *turned
        )
        received = move(send, 0, 1)
        parts = call(
            functools.partial(late_kernel, rows, chips),
            [jax.ShapeDtypeStruct((rows, width), jnp.bfloat16)] * (chips - 1),
            keep,
            received,
            *cores_a,
        )
        arrived.append([move(p, chips - shift, 0) for shift, p in zip(range(1, chips), parts)])
    pieces, scaled = [], None
    for index, (low, high) in enumerate(spans(G_SHARES, depth)):
        shapes = held_shapes(rows, high - low)
        if index == 0:
            scaled, keep, send = call(
                functools.partial(own_kernel, rows, chips),
                [jax.ShapeDtypeStruct((2 * PAD, vocab), jnp.bfloat16), *shapes],
                logits_a,
                *cores_a,
                *turned,
            )
        else:
            keep, send = call(functools.partial(more_own_kernel, rows, low), shapes, scaled, *turned)
        pieces += [keep, move(send, 0, 1), *arrived[index]]

    (stats_b,) = all_logits(ranges_b, parts_b, False)
    chips_b = pair_stats(stats_b)
    grad_a, entropy = call(
        functools.partial(finish_kernel, chips),
        [jax.ShapeDtypeStruct((rows, depth), jnp.bfloat16), jax.ShapeDtypeStruct((rows,), jnp.float32)],
        grad_out[:, None],
        *chips_b,
        *pieces,
    )
    return entropy, grad_a


def solution(mesh):
    chips = mesh.shape["tensor"] // 2
    placed = (
        P(("dp", "tensor"), None),
        P(("dp", "tensor"), None),
        P(("dp", "tensor")),
        P(None, "tensor"),
    )

    def body(*args):
        return per_device(chips, *args)

    return jax.shard_map(
        body,
        mesh=mesh,
        in_specs=placed,
        out_specs=(P(("dp", "tensor")), P(("dp", "tensor"), None)),
        check_vma=False,
    )
```

```python
import functools

import jax
import jax.numpy as jnp
from jax import lax
from jax.experimental import pallas as pl
from jax.experimental.pallas import tpu as pltpu
from jax.sharding import PartitionSpec as P


CHUNK = 1024
PAD = 32
A_SHARES = (8,)
B_SHARES = (6, 2)
G_SHARES = (4, 4)
T_PARTS = 4
VMEM_LIMIT = 24 * 1024 * 1024
STAGE_LIMIT = 40 * 1024 * 1024


def vmem_spec():
    return pl.BlockSpec(memory_space=pltpu.VMEM)


def columns_to_rows(columns):
    count = columns[0].shape[0]
    lane = lax.broadcasted_iota(jnp.int32, (count, 128), 1)
    packed = jnp.zeros((count, 128), jnp.float32)
    for index, column in enumerate(columns):
        packed = jnp.where(lane == index, column, packed)
    return jnp.transpose(packed)[:8]


def rows_to_columns(rows):
    count = rows[0].shape[1]
    sub = lax.broadcasted_iota(jnp.int32, (128, count), 0)
    packed = jnp.zeros((128, count), jnp.float32)
    for index, row in enumerate(rows):
        packed = jnp.where(sub == index, row, packed)
    turned = jnp.transpose(packed)
    return [turned[:, index : index + 1] for index in range(len(rows))]


def spans(shares, depth):
    edges = [0]
    for share in shares:
        edges.append(edges[-1] + depth * share // sum(shares))
    return list(zip(edges, edges[1:]))


def logits_kernel(ranges, slots, more, last, *refs):
    held = len(ranges) * slots
    pieces, weight, sums, outs = refs[:held], refs[held], refs[held + 1 : held + 1 + more], refs[held + 1 + more :]
    logits = sums[0][...] if more else None
    for part, (low, high) in enumerate(ranges):
        for start in range(low, high, CHUNK):
            stop = min(start + CHUNK, high)
            rows = []
            for ref in pieces[part * slots : (part + 1) * slots]:
                offset = start if ref.shape[1] > high - low else start - low
                rows.append(ref[:, offset : offset + stop - start])
                rows.append(jnp.zeros((PAD - ref.shape[0], stop - start), jnp.bfloat16))
            left = jnp.concatenate(rows, axis=0)
            product = jnp.dot(left, weight[start:stop, :], preferred_element_type=jnp.float32)
            logits = product if logits is None else logits + product
    if not last:
        outs[0][...] = logits
        return
    peak = jnp.max(logits, axis=1, keepdims=True)
    shifted = logits - peak
    powers = jnp.exp(shifted)
    total = jnp.sum(powers, axis=1, keepdims=True)
    moment = jnp.sum(powers * shifted, axis=1, keepdims=True)
    outs[0][...] = columns_to_rows([peak, total, moment])
    if len(outs) > 1:
        outs[1][...] = logits
        around = (powers * (shifted - moment / total)).astype(jnp.bfloat16)
        powers = powers.astype(jnp.bfloat16)
        chips = slots // 2
        place = 0
        for first in (1, chips + 1):
            for values in (around, powers):
                size = (chips - 1) * PAD
                outs[2][place : place + size, :] = values[first * PAD : first * PAD + size]
                place += size


def logits_and_stats(ranges, pieces, weight, sums, last, with_logits):
    slots, vocab = len(pieces) // len(ranges), weight.shape[1]
    out = [jax.ShapeDtypeStruct((slots * PAD, vocab), jnp.float32)]
    if last:
        factors = jax.ShapeDtypeStruct((2 * (slots - 2) * PAD, vocab), jnp.bfloat16)
        out = [jax.ShapeDtypeStruct((8, slots * PAD), jnp.float32)] + ([*out, factors] if with_logits else [])
    return call(functools.partial(logits_kernel, ranges, slots, len(sums), last), out, *pieces, weight, *sums)


def align_lanes(stats, shift, flip, chips):
    half = chips * PAD
    if flip:
        stats = pltpu.roll(stats, half, 1)
    move = shift * PAD
    if move:
        lane = lax.broadcasted_iota(jnp.int32, stats.shape, 1) % half
        stats = jnp.where(lane < move, pltpu.roll(stats, (move - half) % (2 * half), 1), pltpu.roll(stats, move, 1))
    return stats


def combine(everyone):
    peak = everyone[0][0:1]
    for stats in everyone[1:]:
        peak = jnp.maximum(peak, stats[0:1])
    total = jnp.zeros_like(peak)
    moment = jnp.zeros_like(peak)
    for stats in everyone:
        below = stats[0:1] - peak
        scale = jnp.exp(below)
        total = total + scale * stats[1:2]
        moment = moment + scale * (stats[2:3] + below * stats[1:2])
    return peak, total, moment


def combine_chips(chips, refs):
    shifted = [align_lanes(ref[...], shift, 0, chips) for shift, ref in enumerate(refs)]
    return combine(shifted)


def pair_stats_kernel(chips, own, mate, out):
    values = combine([own[...], align_lanes(mate[...], 0, 1, chips)])
    out[...] = jnp.concatenate([*values, jnp.zeros((5, out.shape[1]), jnp.float32)], axis=0)


def columns_of(turned, low, width):
    half, start = turned[0].shape[1], low
    while start < low + width:
        stop = min(low + width, (start // half + 1) * half)
        yield start - low, stop - low, turned[start // half][:, start % half : start % half + stop - start]
        start = stop


def early_kernel(rows, low, factors, *refs):
    turned, keep, send = refs[:T_PARTS], refs[-2], refs[-1]
    count = factors.shape[0] // 2
    for start, stop, right in columns_of(turned, low, keep.shape[1]):
        product = jnp.dot(factors[...], right, preferred_element_type=jnp.float32)
        for index in range(count // PAD):
            place = slice(index * rows, (index + 1) * rows)
            near, far = index * PAD, count + index * PAD
            keep[place, start:stop] = product[near : near + rows]
            send[place, start:stop] = product[far : far + rows].astype(jnp.bfloat16)


def late_kernel(rows, chips, keep, received, *refs):
    peak, total, moment = combine_chips(chips, refs[2 : 2 + chips])
    outs = refs[2 + chips :]
    factors = []
    for stats in (refs[0][...], align_lanes(refs[1][...], 0, 1, chips)):
        below = stats[0:1] - peak
        scale = -jnp.exp(below) / total
        factors += [scale, scale * (stats[2:3] / stats[1:2] + below - moment / total)]
    columns = rows_to_columns(factors)
    for slot in range(1, chips):
        total = None
        for which in range(4):
            source = (keep, received)[which // 2]
            place = (which % 2 * (chips - 1) + slot - 1) * rows
            column = columns[which][slot * PAD : slot * PAD + rows]
            term = column * source[place : place + rows, :].astype(jnp.float32)
            total = term if total is None else total + term
        outs[slot - 1][...] = total.astype(jnp.bfloat16)


def own_kernel(rows, chips, logits, *refs):
    stats, turned, outs = refs[:chips], refs[chips:-3], refs[-3:]
    values = rows_to_columns(list(combine_chips(chips, stats)))
    scaled = []
    for first in (0, chips * PAD):
        peak, total, moment = (value[first : first + PAD] for value in values)
        shifted = logits[first : first + PAD, :] - peak
        scaled.append(-(jnp.exp(shifted) / total) * (shifted - moment / total))
    outs[0][...] = jnp.concatenate(scaled, axis=0).astype(jnp.bfloat16)
    more_own_kernel(rows, 0, outs[0], *turned, *outs[1:])


def more_own_kernel(rows, low, scaled, *refs):
    turned, keep, send = refs[:T_PARTS], refs[-2], refs[-1]
    for start, stop, right in columns_of(turned, low, keep.shape[1]):
        product = jnp.dot(scaled[...], right, preferred_element_type=jnp.float32)
        keep[:, start:stop] = product[:rows]
        send[:, start:stop] = product[PAD : PAD + rows].astype(jnp.bfloat16)


def finish_kernel(low, chips, count, factor, *refs):
    parts, stats = refs[: chips + 1], refs[chips + 1 : chips + 1 + count]
    outs = 2 if count else 1
    scratch = refs[len(refs) - outs - 1 :]
    out = refs[len(refs) - 2 * outs - 1]
    semaphores, copies = scratch[-1], []
    if count:
        _, total, moment = combine_chips(chips, stats)
        entropy = refs[len(refs) - 2 * outs]
        scratch[1][...] = (jnp.log(total) - moment / total)[0, : entropy.shape[0]]
        copies.append(pltpu.make_async_copy(scratch[1], entropy, semaphores.at[1]))
        copies[0].start()
    total = parts[0][...]
    for part in parts[1:]:
        total = total + part[...].astype(jnp.float32)
    scratch[0][...] = (factor[...] * total).astype(jnp.bfloat16)
    copies.append(
        pltpu.make_async_copy(scratch[0], out.at[:, pl.ds(low, total.shape[1])], semaphores.at[0])
    )
    copies[-1].start()
    for copy in copies:
        copy.wait()


def finish(low, chips, depth, factor, parts, stats, previous):
    rows, width = parts[0].shape
    anywhere = pl.BlockSpec(memory_space=pl.ANY)
    shapes = [jax.ShapeDtypeStruct((rows, depth), jnp.bfloat16)]
    scratch = [pltpu.VMEM((rows, width), jnp.bfloat16)]
    if stats:
        shapes.append(jax.ShapeDtypeStruct((rows,), jnp.float32))
        scratch.append(pltpu.VMEM((rows,), jnp.float32))
    inputs = [factor, *parts, *stats]
    return pl.pallas_call(
        functools.partial(finish_kernel, low, chips, len(stats)),
        out_shape=shapes,
        in_specs=[vmem_spec()] * len(inputs) + [anywhere] * len(previous),
        out_specs=[anywhere] * len(shapes),
        scratch_shapes=[*scratch, pltpu.SemaphoreType.DMA((2,))],
        input_output_aliases={len(inputs): 0} if previous else {},
        compiler_params=pltpu.CompilerParams(vmem_limit_bytes=VMEM_LIMIT),
        name="finish",
    )(*inputs, *previous)


def held_shapes(rows, width):
    return [jax.ShapeDtypeStruct((rows, width), jnp.float32), jax.ShapeDtypeStruct((rows, width), jnp.bfloat16)]


def call(kernel, out, *args):
    return pl.pallas_call(
        kernel,
        out_shape=out,
        in_specs=[vmem_spec()] * len(args),
        out_specs=jax.tree.map(lambda _: vmem_spec(), out),
        compiler_params=pltpu.CompilerParams(vmem_limit_bytes=VMEM_LIMIT),
    )(*args)


def stage_kernel(weight, out, semaphores):
    steps = semaphores.shape[0]
    step = out.shape[0] // steps
    copies = []
    for index in range(steps):
        part = pl.ds(index * step, step)
        copies.append(pltpu.make_async_copy(weight.at[part, :], out.at[part, :], semaphores.at[index]))
        copies[-1].start()
    for copy in copies:
        copy.wait()


def stage(weight):
    return pl.pallas_call(
        stage_kernel,
        out_shape=jax.ShapeDtypeStruct(weight.shape, weight.dtype),
        in_specs=[pl.BlockSpec(memory_space=pl.ANY)],
        out_specs=vmem_spec(),
        scratch_shapes=[pltpu.SemaphoreType.DMA((4,))],
        compiler_params=pltpu.CompilerParams(vmem_limit_bytes=STAGE_LIMIT),
        name="stage",
    )(weight)


def turn_kernel(low, weight, turned):
    vocab, size = turned.shape
    for column in range(0, vocab, 256):
        block = min(256, vocab - column)
        one = lax.broadcasted_iota(jnp.int32, (block, block), 0) == lax.broadcasted_iota(jnp.int32, (block, block), 1)
        flipped = lax.dot_general(
            jnp.where(one, 1.0, 0.0).astype(jnp.bfloat16),
            weight[low : low + size, column : column + block],
            (((1,), (1,)), ((), ())),
            preferred_element_type=jnp.float32,
        )
        turned[column : column + block, :] = flipped.astype(jnp.bfloat16)


def per_device(chips, hidden_a, hidden_b, grad_out, head_weight):
    rows, depth = hidden_a.shape

    def move(array, shift, flip):
        pairs = [
            (2 * chip + core, 2 * ((chip + shift) % chips) + (core ^ flip)) for chip in range(chips) for core in range(2)
        ]
        return lax.ppermute(array, "tensor", pairs)

    def pair_stats(stats):
        mate = move(stats, 0, 1)
        chip = call(
            functools.partial(pair_stats_kernel, chips), jax.ShapeDtypeStruct(stats.shape, jnp.float32), stats, mate
        )
        return [chip] + [move(chip, shift, 0) for shift in range(1, chips)], mate

    def gather(hidden, shares):
        ranges, parts = spans(shares, depth), []
        own = [hidden if high - low == depth else hidden[:, low:high] for low, high in ranges]
        mate = move(hidden, 0, 1)
        for piece in own:
            across = [move(piece, shift, 0) for shift in range(1, chips)]
            relayed = [move(p, 0, 1) for p in across]
            parts.append([hidden, *across, mate, *relayed])
        return ranges, parts

    ranges_a, parts_a = gather(hidden_a, A_SHARES)
    ranges_b, parts_b = gather(hidden_b, B_SHARES)
    vocab = head_weight.shape[1]
    weight = stage(head_weight)
    turned, size = [], depth // T_PARTS
    for index in range(T_PARTS):
        turned.append(
            call(
                functools.partial(turn_kernel, index * size), jax.ShapeDtypeStruct((vocab, size), weight.dtype), weight
            )
        )

    def all_logits(ranges, parts, with_logits):
        sums = []
        for index, (span, part) in enumerate(zip(ranges, parts)):
            sums = logits_and_stats([span], part, weight, sums, index == len(parts) - 1, with_logits)
        return sums

    stats_a, logits_a, factors_a = all_logits(ranges_a, parts_a, True)
    chips_a, mate_stats_a = pair_stats(stats_a)
    late_stats = [stats_a, mate_stats_a, *chips_a]

    arrived = []
    for low, high in spans(G_SHARES, depth):
        width = high - low
        keep, send = call(
            functools.partial(early_kernel, rows, low), held_shapes(2 * (chips - 1) * rows, width), factors_a, *turned
        )
        received = move(send, 0, 1)
        parts = call(
            functools.partial(late_kernel, rows, chips),
            [jax.ShapeDtypeStruct((rows, width), jnp.bfloat16)] * (chips - 1),
            keep,
            received,
            *late_stats,
        )
        arrived.append([move(p, chips - shift, 0) for shift, p in zip(range(1, chips), parts)])
    pieces, scaled = [], None
    for index, (low, high) in enumerate(spans(G_SHARES, depth)):
        shapes = held_shapes(rows, high - low)
        if index == 0:
            scaled, keep, send = call(
                functools.partial(own_kernel, rows, chips),
                [jax.ShapeDtypeStruct((2 * PAD, vocab), jnp.bfloat16), *shapes],
                logits_a,
                *chips_a,
                *turned,
            )
        else:
            keep, send = call(functools.partial(more_own_kernel, rows, low), shapes, scaled, *turned)
        pieces.append([keep, move(send, 0, 1), *arrived[index]])

    (stats_b,) = all_logits(ranges_b, parts_b, False)
    chips_b, _ = pair_stats(stats_b)
    results = []
    for index, (low, _) in enumerate(spans(G_SHARES, depth)):
        last = index == len(G_SHARES) - 1
        results = finish(
            low, chips, depth, grad_out[:, None], pieces[index], chips_b if last else [], results[:1]
        )
    grad_a, entropy = results
    return entropy, grad_a


def solution(mesh):
    chips = mesh.shape["tensor"] // 2
    placed = (
        P(("dp", "tensor"), None),
        P(("dp", "tensor"), None),
        P(("dp", "tensor")),
        P(None, "tensor"),
    )

    def body(*args):
        return per_device(chips, *args)

    return jax.shard_map(
        body,
        mesh=mesh,
        in_specs=placed,
        out_specs=(P(("dp", "tensor")), P(("dp", "tensor"), None)),
        check_vma=False,
    )
```
